32 devices in a mesh: dp: 8 (over z, y), group: 4 (over x, core).
Axes of the slice: x: 2, y: 2, z: 4, core: 2. Of those that a mesh axis runs over, the one named last changes fastest.
Arguments:
- images: bfloat16 [1536, 768], P(('dp', 'group')), may hold values from -1.5 to 1.5, as said below
- texts: bfloat16 [1536, 768], P(('dp', 'group')), may hold values from -1.5 to 1.5
- send_pos: int32 [4, 384], P('group'), may hold values from 0 to 95, as said below
- recv_slot: int32 [32, 4, 3], P(('dp', 'group')), may hold values from 0 to 7, as said below
- counts: int32 [32, 4], P(('dp', 'group')), may hold values from 1 to 3, as said below
Outputs:
- image_grads: float32 [1536, 768], P(('dp', 'group'))
- caption_grads: float32 [256, 768], P(('dp', 'group'))
The draws below stay inside these ranges and needn't reach their ends.
Inputs may be any that keep to these rules, and one draw needn't show every extreme that they name: `send_pos`: row g lists the pairs of group index g in order of dp index, then row. A position o * 3 + k addresses owner device o (dp index times 4 plus group index); pairs of one caption share a position; in each row every position with k < counts[o, g] is named by at least one pair, and no other position is named. `recv_slot`: the 3 entries of one owner and one sending group are different slots. `counts`: in every group index some owner receives 3 rows. `images`: rows of representations; a caption's text row and its image row are correlated.
All inputs are finite; a program needn't handle non-finite values.
Results may differ from the reference program's by a relative error of at most 0.0026.
Values may be sent and summed in bfloat16 or wider, within the bound.
A program may use at most 128 MiB of HBM per device.

```python
import math
import jax
import jax.numpy as jnp
from jax import lax

EMBED = 768
PAIRS_DEV = 48
CAP = 3
SLOTS = 8
PAIRS = 1536
N_DP = 8
N_GROUP = 4


def pair_draw(key):
    keys = jax.random.split(jax.random.fold_in(key, 17), 5)
    base = jax.random.normal(keys[0], (PAIRS, EMBED), jnp.float32)
    noise = jax.random.normal(keys[1], (PAIRS, EMBED), jnp.float32)
    base = base / math.sqrt(EMBED)
    noise = noise / math.sqrt(EMBED)
    text_scale = jnp.exp(jax.random.uniform(keys[2], (PAIRS, 1), jnp.float32, math.log(0.4), math.log(2.0)))
    image_scale = jnp.exp(jax.random.uniform(keys[3], (PAIRS, 1), jnp.float32, math.log(0.4), math.log(2.0)))
    matching = jax.random.uniform(keys[4], (PAIRS, 1), jnp.float32, 0.5, 1.0)
    texts = base * text_scale
    images = (matching * base + 0.6 * noise) * image_scale
    return (jnp.clip(images, -1.5, 1.5), jnp.clip(texts, -1.5, 1.5))


def draw_images(key, part):
    return pair_draw(key)[0].astype(jnp.bfloat16)


def draw_texts(key, part):
    return pair_draw(key)[1].astype(jnp.bfloat16)


def route_tables(key):
    owner_count = N_DP * N_GROUP
    column_count = N_DP * PAIRS_DEV
    position_count = owner_count * CAP
    keys = jax.random.split(jax.random.fold_in(key, 29), 5)
    heavy = jax.random.randint(keys[0], (owner_count, N_GROUP), 0, 8) == 0
    light = jax.random.randint(keys[1], (owner_count, N_GROUP), 1, CAP)
    group_counts = jnp.where(heavy, CAP, light).astype(jnp.int32)
    fullest = jax.random.randint(keys[2], (N_GROUP,), 0, owner_count)
    group_counts = group_counts.at[fullest, jnp.arange(N_GROUP)].set(CAP)
    group_keys = jax.random.split(keys[3], N_GROUP)

    def one_group(group_key, owner_counts):
        rank_key, extra_key = jax.random.split(group_key)
        valid = (jnp.arange(CAP)[None, :] < owner_counts[:, None]).reshape(position_count)
        ordering = jnp.argsort(jnp.where(valid, 0, 1).astype(jnp.int32), stable=True).astype(jnp.int32)
        used = jnp.sum(valid.astype(jnp.int32))
        ranks = jax.random.permutation(rank_key, column_count).astype(jnp.int32)
        extra = jax.random.randint(extra_key, (column_count,), 0, used)
        picked = jnp.where(ranks < used, ranks, extra)
        return ordering[picked].astype(jnp.int32)
    positions = jax.vmap(one_group)(group_keys, group_counts.T)
    scores = jax.random.randint(keys[4], (owner_count, N_GROUP, SLOTS), 0, 1 << 20) * SLOTS + jnp.arange(SLOTS)
    slot_table = jnp.argsort(scores, axis=-1)[:, :, :CAP].astype(jnp.int32)
    return (positions, slot_table, group_counts)


def draw_send_pos(key, part):
    return route_tables(key)[0]


def draw_recv_slot(key, part):
    return route_tables(key)[1]


def draw_counts(key, part):
    return route_tables(key)[2]


def setup_inputs(seed: int = 0) -> dict:
    splits = jax.random.split(jax.random.key(seed), 6)
    images = draw_images(jax.random.fold_in(splits[5], 71), 0)
    texts = draw_texts(jax.random.fold_in(splits[5], 71), 0)
    send_pos = draw_send_pos(jax.random.fold_in(splits[5], 71), 0)
    recv_slot = draw_recv_slot(jax.random.fold_in(splits[5], 71), 0)
    counts = draw_counts(jax.random.fold_in(splits[5], 71), 0)
    return {"images": images, "texts": texts, "send_pos": send_pos, "recv_slot": recv_slot, "counts": counts}


LOGIT_SCALE = 14.285714

def reference(images, texts, send_pos, recv_slot, counts):
    pair_count = images.shape[0]
    block_rows = math.gcd(512, pair_count)
    block_count = pair_count // block_rows
    image_blocks = images.reshape(block_count, block_rows, EMBED)

    def stats_step(carry, image_block):
        column_high, column_total = carry
        logits = LOGIT_SCALE * jnp.dot(image_block.astype(jnp.float32), texts.T.astype(jnp.float32), preferred_element_type=jnp.float32)
        row_high = jnp.max(logits, axis=1)
        row_norms = row_high + jnp.log(jnp.sum(jnp.exp(logits - row_high[:, None]), axis=1))
        new_high = jnp.maximum(column_high, jnp.max(logits, axis=0))
        column_total = column_total * jnp.exp(column_high - new_high) + jnp.sum(jnp.exp(logits - new_high[None, :]), axis=0)
        return ((new_high, column_total), row_norms)
    start_high = jnp.full((pair_count,), -jnp.inf, jnp.float32)
    start_total = jnp.zeros((pair_count,), jnp.float32)
    (column_high, column_total), row_norms = lax.scan(stats_step, (start_high, start_total), image_blocks)
    column_norms = column_high + jnp.log(column_total)
    pair_index = jnp.arange(pair_count, dtype=jnp.int32)
    first_rows = jnp.arange(block_count, dtype=jnp.int32) * block_rows

    def grad_step(text_total, inputs):
        image_block, block_norms, first_row = inputs
        logits = LOGIT_SCALE * jnp.dot(image_block.astype(jnp.float32), texts.T.astype(jnp.float32), preferred_element_type=jnp.float32)
        diagonal = ((first_row + jnp.arange(block_rows, dtype=jnp.int32))[:, None] == pair_index[None, :]).astype(jnp.float32)
        weights = (0.5 * jnp.exp(logits - block_norms[:, None]) + 0.5 * jnp.exp(logits - column_norms[None, :]) - diagonal).astype(jnp.bfloat16)
        image_part = LOGIT_SCALE * jnp.dot(weights.astype(jnp.float32), texts.astype(jnp.float32), preferred_element_type=jnp.float32)
        text_total = text_total + jnp.dot(weights.T.astype(jnp.float32), image_block.astype(jnp.float32), preferred_element_type=jnp.float32)
        return (text_total, image_part)
    text_start = jnp.zeros((pair_count, EMBED), jnp.float32)
    text_total, image_parts = lax.scan(grad_step, text_start, (image_blocks, row_norms.reshape(block_count, block_rows), first_rows))
    image_grads = image_parts.reshape(pair_count, EMBED)
    text_grads = LOGIT_SCALE * text_total
    device = pair_index // PAIRS_DEV
    data_index = device // N_GROUP
    group_index = device % N_GROUP
    column = data_index * PAIRS_DEV + pair_index % PAIRS_DEV
    position = send_pos[group_index, column]
    owner = position // CAP
    within = position % CAP
    live_rows = within < counts[owner, group_index]
    slot_index = recv_slot[owner, group_index, within]
    target = (owner * SLOTS + slot_index).astype(jnp.int32)
    kept = jnp.where(live_rows[:, None], text_grads, jnp.zeros_like(text_grads))
    caption_grads = jax.ops.segment_sum(kept, target, num_segments=N_DP * N_GROUP * SLOTS)
    return (image_grads, caption_grads)
```

```python
import functools

import jax
import jax.numpy as jnp
from jax import lax
from jax.experimental import pallas as pl
from jax.experimental.pallas import tpu as pltpu
from jax.sharding import PartitionSpec as P

CAP = 3
SLOTS = 8
PAD = 4
LOGIT_SCALE = 14.285714
MESH = pl.DeviceIdType.MESH
F32 = jnp.float32
BF16 = jnp.bfloat16


def loop(count, body):
    if count <= 8:
        for step in range(count):
            body(step)
    else:
        lax.fori_loop(0, count, lambda step, _: (body(step), 0)[1], 0)


def dot_nt(left, right):
    return lax.dot_general(left, right, (((1,), (1,)), ((), ())), preferred_element_type=F32)


def dot_nn(left, right):
    return lax.dot_general(left, right, (((1,), (0,)), ((), ())), preferred_element_type=F32)


def merge_lse(parts):
    high = functools.reduce(jnp.maximum, parts)
    return high + jnp.log(functools.reduce(jnp.add, [jnp.exp(part - high) for part in parts]))


def kernel(
    dp_count, group_count, columns, images, texts, send_pos, recv_slot, counts,
    image_grads, caption_grads,
    image_all, text_all, logits, row_high, row_total, row_lse, column_lse, own_row, own_column,
    weights, part_send, part_recv, cap_send, cap_recv,
    image_send_sem, image_recv_sem, text_send_sem, text_recv_sem,
    row_send_sem, row_recv_sem, column_send_sem, column_recv_sem,
    part_send_sem, part_recv_sem, cap_send_sem, cap_recv_sem,
):
    rows = images.shape[0]
    width = images.shape[1]
    block_rows = group_count * rows
    chunk_count = dp_count * rows // columns
    device_count = dp_count * group_count
    d = lax.axis_index("dp")
    g = lax.axis_index("group")
    me = d * group_count + g
    twin = d + 1 - 2 * (d % 2)
    half = dp_count // 2

    def peer_dp(step):
        return (d + 1 + step) % dp_count

    def peer_group(step):
        return (g + 1 + step) % group_count

    def peer_same(step):
        return ((d // 2 + 1 + step) % half) * 2 + d % 2

    def wait_bytes(ref, sem):
        pltpu.make_async_copy(ref, ref, sem).wait()

    barrier = pltpu.get_barrier_semaphore()
    loop(dp_count - 1, lambda step: pl.semaphore_signal(
        barrier, inc=1, device_id=(peer_dp(step), g), device_id_type=MESH))
    loop(group_count - 1, lambda step: pl.semaphore_signal(
        barrier, inc=1, device_id=(d, peer_group(step)), device_id_type=MESH))

    own_image_rows = pl.ds(pl.multiple_of(g * rows, 16), rows)
    own_text_rows = pl.ds(pl.multiple_of(d * rows, 16), rows)
    image_all[own_image_rows, :] = images[...]
    text_all[own_text_rows, :] = texts[...]
    pl.semaphore_wait(barrier, dp_count + group_count - 2)

    def text_rows(source):
        return text_all.at[pl.ds(pl.multiple_of(source * rows, 16), rows), :]

    def text_copy(source_ref, source, target):
        return pltpu.make_async_remote_copy(
            src_ref=source_ref, dst_ref=text_rows(source),
            send_sem=text_send_sem.at[0], recv_sem=text_recv_sem.at[source],
            device_id=(target, g), device_id_type=MESH)

    loop(half - 1, lambda step: text_copy(texts, d, peer_same(step)).start())
    text_copy(texts, d, twin).start()

    def image_copy(step):
        return pltpu.make_async_remote_copy(
            src_ref=images, dst_ref=image_all.at[own_image_rows, :],
            send_sem=image_send_sem.at[0], recv_sem=image_recv_sem.at[0],
            device_id=(d, peer_group(step)), device_id_type=MESH)

    loop(group_count - 1, lambda step: image_copy(step).start())

    def arrived(source):
        text_copy(texts, source, twin).wait_recv()

    def forward(step):
        source = (d // 2 + half - 1 - step) % half * 2 + d % 2
        arrived(source)
        text_copy(text_rows(source), source, twin).start()

    loop(half - 1, forward)
    loop(half, lambda step: arrived((twin // 2 + half - step) % half * 2 + twin % 2))
    wait_bytes(image_all.at[pl.ds(0, (group_count - 1) * rows), :], image_recv_sem.at[0])

    row_high[...] = jnp.full_like(row_high, -jnp.inf)
    row_total[...] = jnp.zeros_like(row_total)

    def columns_of(chunk):
        return pl.ds(pl.multiple_of(chunk * columns, 128), columns)

    def text_chunk(chunk):
        return text_all[pl.ds(pl.multiple_of(chunk * columns, 16), columns), :]

    def logit_step(chunk):
        block = LOGIT_SCALE * dot_nt(image_all[...], text_chunk(chunk))
        logits[chunk] = block
        row_high[...] = jnp.maximum(row_high[...], jnp.max(block, axis=1, keepdims=True))
        high = jnp.max(block, axis=0, keepdims=True)
        own_column[:, columns_of(chunk)] = high + jnp.log(
            jnp.sum(jnp.exp(block - high), axis=0, keepdims=True))

    loop(chunk_count, logit_step)

    def column_copy(step):
        return pltpu.make_async_remote_copy(
            src_ref=own_column, dst_ref=column_lse.at[d],
            send_sem=column_send_sem.at[0], recv_sem=column_recv_sem.at[0],
            device_id=(peer_dp(step), g), device_id_type=MESH)

    loop(dp_count - 1, lambda step: column_copy(step).start())
    column_lse[d] = own_column[...]

    def total_step(chunk):
        row_total[...] += jnp.sum(jnp.exp(logits[chunk] - row_high[...]), axis=1, keepdims=True)

    loop(chunk_count, total_step)
    diagonal = (
        lax.broadcasted_iota(jnp.int32, (block_rows, block_rows), 0)
        == lax.broadcasted_iota(jnp.int32, (block_rows, block_rows), 1)
    )
    lse = row_high[...] + jnp.log(row_total[...])
    own_row[...] = jnp.sum(jnp.where(diagonal, lse, 0.0), axis=0, keepdims=True)

    def row_copy(step):
        return pltpu.make_async_remote_copy(
            src_ref=own_row, dst_ref=row_lse.at[g],
            send_sem=row_send_sem.at[0], recv_sem=row_recv_sem.at[0],
            device_id=(d, peer_group(step)), device_id_type=MESH)

    loop(group_count - 1, lambda step: row_copy(step).start())
    row_lse[g] = own_row[...]
    wait_bytes(row_lse.at[pl.ds(0, group_count - 1)], row_recv_sem.at[0])
    row_norm = merge_lse([row_lse[source] for source in range(group_count)])
    row_norm = jnp.sum(jnp.where(diagonal, row_norm, 0.0), axis=1, keepdims=True)
    row_high[...] = row_norm
    wait_bytes(column_lse.at[pl.ds(0, dp_count - 1)], column_recv_sem.at[0])

    def weight_step(chunk):
        where = columns_of(chunk)
        column_norm = merge_lse([column_lse[source, :, where] for source in range(dp_count)])
        block = logits[chunk]
        row = lax.broadcasted_iota(jnp.int32, block.shape, 0) - g * rows
        column = lax.broadcasted_iota(jnp.int32, block.shape, 1) + (chunk * columns - d * rows)
        same = (row == column) & (row >= 0) & (row < rows)
        weights[chunk] = (
            0.5 * jnp.exp(block - row_high[...])
            + 0.5 * jnp.exp(block - column_norm)
            - same.astype(F32)
        ).astype(BF16)

    loop(chunk_count, weight_step)

    owner_block = 32
    merged_rows = owner_block * PAD

    def caption_step(step):
        index = lax.broadcasted_iota(jnp.int32, (merged_rows, columns), 0)
        within = index % PAD
        position = jnp.where(
            within < CAP, (step * owner_block + index // PAD) * CAP + within, -1)
        merged = jnp.zeros((merged_rows, block_rows), F32)
        if chunk_count == 1:
            chosen = (send_pos[...] == position).astype(BF16)
            merged = dot_nt(chosen, weights[0])
        else:
            def add(chunk, total):
                chosen = (send_pos[:, columns_of(chunk)] == position).astype(BF16)
                return total + dot_nt(chosen, weights[chunk])
            merged = lax.fori_loop(0, chunk_count, add, merged)
        coarse = merged.astype(BF16)
        fine = (merged - coarse.astype(F32)).astype(BF16)
        block = LOGIT_SCALE * (dot_nn(coarse, image_all[...]) + dot_nn(fine, image_all[...]))
        cap_send[pl.ds(step * owner_block, owner_block)] = block.reshape(
            owner_block, PAD, width).astype(BF16)

    loop(device_count // owner_block, caption_step)

    def cap_copy(step):
        target = (me + 1 + step) % device_count
        return pltpu.make_async_remote_copy(
            src_ref=cap_send.at[target], dst_ref=cap_recv.at[me],
            send_sem=cap_send_sem.at[0], recv_sem=cap_recv_sem.at[0],
            device_id=(target // group_count, target % group_count), device_id_type=MESH)

    lax.fori_loop(0, device_count - 1, lambda step, _: (cap_copy(step).start(), 0)[1], 0)
    cap_recv[me] = cap_send[me]

    if chunk_count == 1:
        part = dot_nn(weights[0], text_chunk(0))
    else:
        part = lax.fori_loop(
            0, chunk_count,
            lambda chunk, total: total + dot_nn(weights[chunk], text_chunk(chunk)),
            jnp.zeros((block_rows, width), F32))
    part = LOGIT_SCALE * part
    for target in range(group_count):
        part_send[target] = part[target * rows:(target + 1) * rows].astype(BF16)

    def part_copy(step):
        target = peer_group(step)
        return pltpu.make_async_remote_copy(
            src_ref=part_send.at[target], dst_ref=part_recv.at[g],
            send_sem=part_send_sem.at[0], recv_sem=part_recv_sem.at[0],
            device_id=(d, target), device_id_type=MESH)

    loop(group_count - 1, lambda step: part_copy(step).start())
    part_recv[g] = part_send[g]
    wait_bytes(part_recv.at[pl.ds(0, group_count - 1)], part_recv_sem.at[0])
    image_grads[...] = functools.reduce(
        jnp.add, [part_recv[source].astype(F32) for source in range(group_count)])

    wait_bytes(cap_recv.at[pl.ds(0, device_count - 1)], cap_recv_sem.at[0])
    slot = lax.broadcasted_iota(jnp.int32, (SLOTS, width), 0)
    result = jnp.zeros((SLOTS, width), F32)
    for source in range(group_count):
        if dp_count <= 8:
            total = functools.reduce(
                jnp.add,
                [cap_recv[q * group_count + source].astype(F32) for q in range(dp_count)])
        else:
            total = lax.fori_loop(
                0, dp_count,
                lambda q, total: total + cap_recv[q * group_count + source].astype(F32),
                jnp.zeros((PAD, width), F32))
        for k in range(CAP):
            live = k < counts[0, source]
            chosen = jnp.where(live, recv_slot[0, source, k], SLOTS)
            result = result + jnp.where(slot == chosen, total[k:k + 1], 0.0)
    caption_grads[...] = result

    wait_bytes(text_all.at[pl.ds(0, (dp_count - 1) * rows), :], text_send_sem.at[0])
    wait_bytes(image_all.at[pl.ds(0, (group_count - 1) * rows), :], image_send_sem.at[0])
    wait_bytes(column_lse.at[pl.ds(0, dp_count - 1)], column_send_sem.at[0])
    wait_bytes(row_lse.at[pl.ds(0, group_count - 1)], row_send_sem.at[0])
    wait_bytes(part_recv.at[pl.ds(0, group_count - 1)], part_send_sem.at[0])
    wait_bytes(cap_recv.at[pl.ds(0, device_count - 1)], cap_send_sem.at[0])


def on_device(dp_count, group_count, images, texts, send_pos, recv_slot, counts):
    rows, width = images.shape
    block_rows = group_count * rows
    total = dp_count * rows
    columns = min(dp_count, 8) * rows
    chunks = total // columns
    devices = dp_count * group_count
    vmem = pl.BlockSpec(memory_space=pltpu.VMEM)
    smem = pl.BlockSpec(memory_space=pltpu.SMEM)
    dma = pltpu.SemaphoreType.DMA
    return pl.pallas_call(
        functools.partial(kernel, dp_count, group_count, columns),
        out_shape=(
            jax.ShapeDtypeStruct((rows, width), F32),
            jax.ShapeDtypeStruct((SLOTS, width), F32),
        ),
        in_specs=[vmem, vmem, vmem, smem, smem],
        out_specs=(vmem, vmem),
        scratch_shapes=[
            pltpu.VMEM((block_rows, width), BF16),
            pltpu.VMEM((total, width), BF16),
            pltpu.VMEM((chunks, block_rows, columns), F32),
            pltpu.VMEM((block_rows, 1), F32),
            pltpu.VMEM((block_rows, 1), F32),
            pltpu.VMEM((group_count, 1, block_rows), F32),
            pltpu.VMEM((dp_count, 1, total), F32),
            pltpu.VMEM((1, block_rows), F32),
            pltpu.VMEM((1, total), F32),
            pltpu.VMEM((chunks, block_rows, columns), BF16),
            pltpu.VMEM((group_count, rows, width), BF16),
            pltpu.VMEM((group_count, rows, width), BF16),
            pltpu.VMEM((devices, PAD, width), BF16),
            pltpu.VMEM((devices, PAD, width), BF16),
            dma((1,)), dma((1,)), dma((1,)), dma((dp_count,)),
            dma((1,)), dma((1,)), dma((1,)), dma((1,)),
            dma((1,)), dma((1,)), dma((1,)), dma((1,)),
        ],
        compiler_params=pltpu.CompilerParams(
            collective_id=0, has_side_effects=True, vmem_limit_bytes=60 * 1024 * 1024),
    )(images, texts, send_pos, recv_slot, counts)


def solution(mesh):
    placed = (
        P(("dp", "group"), None),
        P(("dp", "group"), None),
        P("group", None),
        P(("dp", "group"), None, None),
        P(("dp", "group"), None),
    )
    return jax.shard_map(
        functools.partial(on_device, mesh.shape["dp"], mesh.shape["group"]),
        mesh=mesh,
        in_specs=placed,
        out_specs=(P(("dp", "group"), None), P(("dp", "group"), None)),
        check_vma=False,
    )
```

```python
import functools

import jax
import jax.numpy as jnp
from jax import lax
from jax.experimental import pallas as pl
from jax.experimental.pallas import tpu as pltpu
from jax.sharding import PartitionSpec as P

CAP = 3
SLOTS = 8
PAD = 4
LOGIT_SCALE = 14.285714
MESH = pl.DeviceIdType.MESH
F32 = jnp.float32
BF16 = jnp.bfloat16


def loop(count, body):
    if count <= 8:
        for step in range(count):
            body(step)
    else:
        lax.fori_loop(0, count, lambda step, _: (body(step), 0)[1], 0)


def dot_nt(left, right):
    return lax.dot_general(left, right, (((1,), (1,)), ((), ())), preferred_element_type=F32)


def dot_nn(left, right):
    return lax.dot_general(left, right, (((1,), (0,)), ((), ())), preferred_element_type=F32)


def merge_lse(parts):
    high = functools.reduce(jnp.maximum, parts)
    return high + jnp.log(functools.reduce(jnp.add, [jnp.exp(part - high) for part in parts]))


def kernel(
    dp_count, group_count, columns, images_in, texts_in, send_pos_in, recv_slot_in, counts_in,
    image_grads, caption_grads,
    images, texts, send_pos, recv_slot, counts, load_sem,
    image_all, text_all, logits, row_high, row_total, row_lse, column_lse, own_row, own_column,
    weights, part_own, part_send, part_recv, cap_send, cap_recv,
    image_send_sem, image_recv_sem, text_send_sem, text_recv_sem,
    row_send_sem, row_recv_sem, column_send_sem, column_recv_sem,
    part_send_sem, part_recv_sem, cap_send_sem, cap_recv_sem,
):
    rows = images.shape[0]
    width = images.shape[1]
    block_rows = group_count * rows
    chunk_count = dp_count * rows // columns
    device_count = dp_count * group_count
    d = lax.axis_index("dp")
    g = lax.axis_index("group")
    me = d * group_count + g
    twin = d + 1 - 2 * (d % 2)
    half = dp_count // 2

    def peer_dp(step):
        return (d + 1 + step) % dp_count

    def peer_group(step):
        return (g + 1 + step) % group_count

    def peer_same(step):
        return ((d // 2 + 1 + step) % half) * 2 + d % 2

    def wait_bytes(ref, sem):
        pltpu.make_async_copy(ref, ref, sem).wait()

    barrier = pltpu.get_barrier_semaphore()
    loop(dp_count - 1, lambda step: pl.semaphore_signal(
        barrier, inc=1, device_id=(peer_dp(step), g), device_id_type=MESH))
    loop(group_count - 1, lambda step: pl.semaphore_signal(
        barrier, inc=1, device_id=(d, peer_group(step)), device_id_type=MESH))

    loads = [
        pltpu.make_async_copy(source, target, load_sem.at[index])
        for index, (source, target) in enumerate((
            (texts_in, texts), (images_in, images), (send_pos_in, send_pos),
            (recv_slot_in, recv_slot), (counts_in, counts)))
    ]
    for load in loads:
        load.start()
    for load in loads:
        load.wait()
    own_image_rows = pl.ds(pl.multiple_of(g * rows, 16), rows)
    own_text_rows = pl.ds(pl.multiple_of(d * rows, 16), rows)
    image_all[own_image_rows, :] = images[...]
    text_all[own_text_rows, :] = texts[...]
    pl.semaphore_wait(barrier, dp_count + group_count - 2)

    def text_rows(source):
        return text_all.at[pl.ds(pl.multiple_of(source * rows, 16), rows), :]

    def text_copy(source_ref, source, target):
        return pltpu.make_async_remote_copy(
            src_ref=source_ref, dst_ref=text_rows(source),
            send_sem=text_send_sem.at[0], recv_sem=text_recv_sem.at[source],
            device_id=(target, g), device_id_type=MESH)

    loop(half - 1, lambda step: text_copy(texts, d, peer_same(step)).start())
    text_copy(texts, d, twin).start()

    def image_copy(step):
        return pltpu.make_async_remote_copy(
            src_ref=images, dst_ref=image_all.at[own_image_rows, :],
            send_sem=image_send_sem.at[0], recv_sem=image_recv_sem.at[0],
            device_id=(d, peer_group(step)), device_id_type=MESH)

    loop(group_count - 1, lambda step: image_copy(step).start())

    def arrived(source):
        text_copy(texts, source, twin).wait_recv()

    def forward(step):
        source = (d // 2 + half - 1 - step) % half * 2 + d % 2
        arrived(source)
        text_copy(text_rows(source), source, twin).start()

    loop(half - 1, forward)
    loop(half, lambda step: arrived((twin // 2 + half - step) % half * 2 + twin % 2))
    wait_bytes(image_all.at[pl.ds(0, (group_count - 1) * rows), :], image_recv_sem.at[0])

    row_high[...] = jnp.full_like(row_high, -jnp.inf)
    row_total[...] = jnp.zeros_like(row_total)

    def columns_of(chunk):
        return pl.ds(pl.multiple_of(chunk * columns, 128), columns)

    def text_chunk(chunk):
        return text_all[pl.ds(pl.multiple_of(chunk * columns, 16), columns), :]

    def logit_step(chunk):
        block = LOGIT_SCALE * dot_nt(image_all[...], text_chunk(chunk))
        logits[chunk] = block
        row_high[...] = jnp.maximum(row_high[...], jnp.max(block, axis=1, keepdims=True))
        high = jnp.max(block, axis=0, keepdims=True)
        own_column[:, columns_of(chunk)] = high + jnp.log(
            jnp.sum(jnp.exp(block - high), axis=0, keepdims=True))

    loop(chunk_count, logit_step)

    def column_copy(step):
        return pltpu.make_async_remote_copy(
            src_ref=own_column, dst_ref=column_lse.at[d],
            send_sem=column_send_sem.at[0], recv_sem=column_recv_sem.at[0],
            device_id=(peer_dp(step), g), device_id_type=MESH)

    loop(dp_count - 1, lambda step: column_copy(step).start())
    column_lse[d] = own_column[...]

    def total_step(chunk):
        row_total[...] += jnp.sum(jnp.exp(logits[chunk] - row_high[...]), axis=1, keepdims=True)

    loop(chunk_count, total_step)
    diagonal = (
        lax.broadcasted_iota(jnp.int32, (block_rows, block_rows), 0)
        == lax.broadcasted_iota(jnp.int32, (block_rows, block_rows), 1)
    )
    lse = row_high[...] + jnp.log(row_total[...])
    own_row[...] = jnp.sum(jnp.where(diagonal, lse, 0.0), axis=0, keepdims=True)

    def row_copy(step):
        return pltpu.make_async_remote_copy(
            src_ref=own_row, dst_ref=row_lse.at[g],
            send_sem=row_send_sem.at[0], recv_sem=row_recv_sem.at[0],
            device_id=(d, peer_group(step)), device_id_type=MESH)

    loop(group_count - 1, lambda step: row_copy(step).start())
    row_lse[g] = own_row[...]
    wait_bytes(row_lse.at[pl.ds(0, group_count - 1)], row_recv_sem.at[0])
    row_norm = merge_lse([row_lse[source] for source in range(group_count)])
    row_norm = jnp.sum(jnp.where(diagonal, row_norm, 0.0), axis=1, keepdims=True)
    row_high[...] = row_norm
    wait_bytes(column_lse.at[pl.ds(0, dp_count - 1)], column_recv_sem.at[0])

    def weight_step(chunk):
        where = columns_of(chunk)
        column_norm = merge_lse([column_lse[source, :, where] for source in range(dp_count)])
        block = logits[chunk]
        row = lax.broadcasted_iota(jnp.int32, block.shape, 0) - g * rows
        column = lax.broadcasted_iota(jnp.int32, block.shape, 1) + (chunk * columns - d * rows)
        same = (row == column) & (row >= 0) & (row < rows)
        weights[chunk] = (
            0.5 * jnp.exp(block - row_high[...])
            + 0.5 * jnp.exp(block - column_norm)
            - same.astype(F32)
        ).astype(BF16)

    loop(chunk_count, weight_step)

    owner_block = 32
    merged_rows = owner_block * PAD

    def caption_step(step):
        index = lax.broadcasted_iota(jnp.int32, (merged_rows, columns), 0)
        within = index % PAD
        position = jnp.where(
            within < CAP, (step * owner_block + index // PAD) * CAP + within, -1)
        merged = jnp.zeros((merged_rows, block_rows), F32)
        if chunk_count == 1:
            chosen = (send_pos[...] == position).astype(BF16)
            merged = dot_nt(chosen, weights[0])
        else:
            def add(chunk, total):
                chosen = (send_pos[:, columns_of(chunk)] == position).astype(BF16)
                return total + dot_nt(chosen, weights[chunk])
            merged = lax.fori_loop(0, chunk_count, add, merged)
        coarse = merged.astype(BF16)
        fine = (merged - coarse.astype(F32)).astype(BF16)
        block = LOGIT_SCALE * (dot_nn(coarse, image_all[...]) + dot_nn(fine, image_all[...]))
        cap_send[pl.ds(step * owner_block, owner_block)] = block.reshape(
            owner_block, PAD, width).astype(BF16)

    loop(device_count // owner_block, caption_step)

    def cap_copy(step):
        target = (me + 1 + step) % device_count
        return pltpu.make_async_remote_copy(
            src_ref=cap_send.at[target], dst_ref=cap_recv.at[me],
            send_sem=cap_send_sem.at[0], recv_sem=cap_recv_sem.at[0],
            device_id=(target // group_count, target % group_count), device_id_type=MESH)

    lax.fori_loop(0, device_count - 1, lambda step, _: (cap_copy(step).start(), 0)[1], 0)
    cap_recv[me] = cap_send[me]

    if chunk_count == 1:
        part = dot_nn(weights[0], text_chunk(0))
    else:
        part = lax.fori_loop(
            0, chunk_count,
            lambda chunk, total: total + dot_nn(weights[chunk], text_chunk(chunk)),
            jnp.zeros((block_rows, width), F32))
    part = LOGIT_SCALE * part
    part_own[...] = part
    for target in range(group_count):
        part_send[target] = part[target * rows:(target + 1) * rows].astype(BF16)

    def part_copy(step):
        target = peer_group(step)
        return pltpu.make_async_remote_copy(
            src_ref=part_send.at[target], dst_ref=part_recv.at[g],
            send_sem=part_send_sem.at[0], recv_sem=part_recv_sem.at[0],
            device_id=(d, target), device_id_type=MESH)

    loop(group_count - 1, lambda step: part_copy(step).start())
    part_recv[g] = jnp.zeros((rows, width), BF16)
    wait_bytes(part_recv.at[pl.ds(0, group_count - 1)], part_recv_sem.at[0])
    image_grads[...] = part_own[own_image_rows, :] + functools.reduce(
        jnp.add, [part_recv[source].astype(F32) for source in range(group_count)])

    wait_bytes(cap_recv.at[pl.ds(0, device_count - 1)], cap_recv_sem.at[0])
    slot = lax.broadcasted_iota(jnp.int32, (SLOTS, width), 0)
    result = jnp.zeros((SLOTS, width), F32)
    for source in range(group_count):
        if dp_count <= 8:
            total = functools.reduce(
                jnp.add,
                [cap_recv[q * group_count + source].astype(F32) for q in range(dp_count)])
        else:
            total = lax.fori_loop(
                0, dp_count,
                lambda q, total: total + cap_recv[q * group_count + source].astype(F32),
                jnp.zeros((PAD, width), F32))
        for k in range(CAP):
            live = k < counts[0, source]
            chosen = jnp.where(live, recv_slot[k, 0, source], SLOTS)
            result = result + jnp.where(slot == chosen, total[k:k + 1], 0.0)
    caption_grads[...] = result

    wait_bytes(text_all.at[pl.ds(0, (dp_count - 1) * rows), :], text_send_sem.at[0])
    wait_bytes(image_all.at[pl.ds(0, (group_count - 1) * rows), :], image_send_sem.at[0])
    wait_bytes(column_lse.at[pl.ds(0, dp_count - 1)], column_send_sem.at[0])
    wait_bytes(row_lse.at[pl.ds(0, group_count - 1)], row_send_sem.at[0])
    wait_bytes(part_recv.at[pl.ds(0, group_count - 1)], part_send_sem.at[0])
    wait_bytes(cap_recv.at[pl.ds(0, device_count - 1)], cap_send_sem.at[0])


def on_device(dp_count, group_count, images, texts, send_pos, recv_slot, counts):
    rows, width = images.shape
    block_rows = group_count * rows
    total = dp_count * rows
    columns = min(dp_count, 8) * rows
    chunks = total // columns
    devices = dp_count * group_count
    vmem = pl.BlockSpec(memory_space=pltpu.VMEM)
    anywhere = pl.BlockSpec(memory_space=pl.ANY)
    dma = pltpu.SemaphoreType.DMA
    return pl.pallas_call(
        functools.partial(kernel, dp_count, group_count, columns),
        out_shape=(
            pltpu.VMEM((rows, width), F32),
            pltpu.VMEM((SLOTS, width), F32),
        ),
        in_specs=[anywhere] * 5,
        out_specs=(vmem, vmem),
        scratch_shapes=[
            pltpu.VMEM((rows, width), BF16),
            pltpu.VMEM((rows, width), BF16),
            pltpu.VMEM((1, total), jnp.int32),
            pltpu.SMEM((CAP, 1, group_count), jnp.int32),
            pltpu.SMEM((1, group_count), jnp.int32),
            dma((5,)),
            pltpu.VMEM((block_rows, width), BF16),
            pltpu.VMEM((total, width), BF16),
            pltpu.VMEM((chunks, block_rows, columns), F32),
            pltpu.VMEM((block_rows, 1), F32),
            pltpu.VMEM((block_rows, 1), F32),
            pltpu.VMEM((group_count, 1, block_rows), F32),
            pltpu.VMEM((dp_count, 1, total), F32),
            pltpu.VMEM((1, block_rows), F32),
            pltpu.VMEM((1, total), F32),
            pltpu.VMEM((chunks, block_rows, columns), BF16),
            pltpu.VMEM((block_rows, width), F32),
            pltpu.VMEM((group_count, rows, width), BF16),
            pltpu.VMEM((group_count, rows, width), BF16),
            pltpu.VMEM((devices, PAD, width), BF16),
            pltpu.VMEM((devices, PAD, width), BF16),
            dma((1,)), dma((1,)), dma((1,)), dma((dp_count,)),
            dma((1,)), dma((1,)), dma((1,)), dma((1,)),
            dma((1,)), dma((1,)), dma((1,)), dma((1,)),
        ],
        compiler_params=pltpu.CompilerParams(
            collective_id=0, has_side_effects=True, vmem_limit_bytes=60 * 1024 * 1024),
    )(images, texts, send_pos, jnp.transpose(recv_slot, (2, 0, 1)), counts)


def solution(mesh):
    placed = (
        P(("dp", "group"), None),
        P(("dp", "group"), None),
        P("group", None),
        P(("dp", "group"), None, None),
        P(("dp", "group"), None),
    )
    return jax.shard_map(
        functools.partial(on_device, mesh.shape["dp"], mesh.shape["group"]),
        mesh=mesh,
        in_specs=placed,
        out_specs=(P(("dp", "group"), None), P(("dp", "group"), None)),
        check_vma=False,
    )
```
